32 devices in a mesh: cp: 16 (over z, y, x), hd: 2 (over core).
Axes of the slice: x: 2, y: 2, z: 4, core: 2. Of those that a mesh axis runs over, the one named last changes fastest.
Arguments:
- queries: bfloat16 [3072, 4096], P('cp', 'hd'), may hold values from -48 to 48
- keys: bfloat16 [3072, 1024], P('cp', 'hd'), may hold values from -48 to 48
- values: bfloat16 [3072, 1024], P('cp', 'hd'), may hold values from -6 to 6
- span_table: int32 [32], replicated, may hold values from 0 to 31, as said below
- doc_ids: int32 [3072], replicated, may hold values from 0 to 7, never falling along the last dimension, each value on 1 to 768 neighbouring positions
- out_weight: bfloat16 [4096, 4096], P('hd'), may hold values from -0.09375 to 0.09375
Outputs:
- mixed: bfloat16 [3072, 4096], P(('cp', 'hd'))
The draws below stay inside these ranges and needn't reach their ends.
Inputs may be any that keep to these rules, and one draw needn't show every extreme that they name: `span_table`: slots 2 j and 2 j + 1 hold two spans c and 31 - c, and every span is held once.
All inputs are finite; a program needn't handle non-finite values.
Results may differ from the reference program's by a relative error of at most 0.0095.
Values may be sent and summed in bfloat16 or wider, within the bound.
A program may use at most 128 MiB of HBM per device.

```python
import math
import jax
import jax.numpy as jnp
import numpy as np
from jax import lax

D = 4096
QUERY_HEADS = 32
KEY_VALUE_HEADS = 8
HEAD_WIDTH = 128
SPAN_TOKENS = 96
DOCS = 8
SPANS = 32
SEQUENCE_TOKENS = 3072


def paired_table(key):
    pairs = jax.random.permutation(jax.random.fold_in(key, 11), SPANS // 2).astype(jnp.int32)
    flips = jax.random.randint(jax.random.fold_in(key, 12), (SPANS // 2,), 0, 2)
    upper = (SPANS - 1 - pairs).astype(jnp.int32)
    first = jnp.where(flips == 1, upper, pairs)
    second = jnp.where(flips == 1, pairs, upper)
    return jnp.stack([first, second], axis=1).reshape(SPANS).astype(jnp.int32)


def draw_span_table(key, part):
    return paired_table(key)


def drawn_pair(key):
    drawn_key_rows = jnp.clip(jax.random.normal(jax.random.fold_in(key, 21), (SEQUENCE_TOKENS, KEY_VALUE_HEADS * HEAD_WIDTH), jnp.float32), -6.0, 6.0)
    base_queries = jnp.clip(jax.random.normal(jax.random.fold_in(key, 22), (SEQUENCE_TOKENS, QUERY_HEADS * HEAD_WIDTH), jnp.float32), -6.0, 6.0)
    new_keys = drawn_key_rows
    new_queries = base_queries
    return (jnp.clip(new_queries, -48.0, 48.0), jnp.clip(new_keys, -48.0, 48.0))


def draw_queries(key, part):
    return drawn_pair(key)[0].astype(jnp.bfloat16)


def draw_keys(key, part):
    return drawn_pair(key)[1].astype(jnp.bfloat16)


def block_levels(rng, dims, shards, smallest, high):
    def one(dim, blocks):
        steps = jax.random.uniform(jax.random.fold_in(jax.random.fold_in(rng, 6), dim), (blocks,), jnp.float32, smallest / len(shards), high / len(shards))
        return jnp.repeat(jnp.exp(steps), dims[dim] // blocks).reshape((-1,) + (1,) * (len(dims) - dim - 1))

    gain = one(*shards[0])
    for cut in shards[1:]:
        gain = gain * one(*cut)
    return gain


def split_up(amount, total, bound, slope):
    portions = [(1 << 20) // math.isqrt(rank ** slope) + 1 for rank in range(2, amount + 1)]
    surplus, given = total - bound - (amount - 1), [1] * (amount - 1)
    while surplus > 0:
        movable = [i for i in range(amount - 1) if given[i] < bound]
        pool, left = sum([portions[i] for i in movable]), surplus
        for i in movable:
            extra = min(bound - given[i], max(1, left * portions[i] // pool), surplus)
            given[i] = given[i] + extra
            surplus = surplus - extra
    return np.array([bound] + given)


def ragged_sizes(own_key, count, total, limit, lean):
    if count == 2:
        one = jax.random.randint(own_key, (), max(1, total - limit), min(limit, total - 1) + 1)
        return jnp.stack([one, total - one])
    sizes = jnp.asarray(split_up(count, total, limit, lean), jnp.int32)
    twos = (count - 1) // 2
    source_of, taker = sizes[1:1 + 2 * twos:2], sizes[2:2 + 2 * twos:2]
    room = jnp.minimum(source_of - 1, limit - taker)
    moved = jax.random.randint(jax.random.fold_in(own_key, 1), (twos,), 0, 1 << 20) % (room + 1)
    sizes = sizes.at[1:1 + 2 * twos:2].set(source_of - moved).at[2:2 + 2 * twos:2].set(taker + moved)
    return sizes[jax.random.permutation(jax.random.fold_in(own_key, 2), count)]


def centred(key, dims, width, bound, cuts=(), kind=jnp.bfloat16):
    gain = block_levels(key, dims, cuts, -0.22, 0.18) if cuts else 1.0
    values = jax.random.normal(key, dims, jnp.float32) * width * gain
    return jnp.minimum(jnp.maximum(values, -bound), bound).astype(kind)


def setup_inputs(seed: int = 0) -> dict:
    seeds = jax.random.split(jax.random.key(seed), 7)
    return {
        "queries": draw_queries(jax.random.fold_in(seeds[6], 71), 0),
        "keys": draw_keys(jax.random.fold_in(seeds[6], 71), 0),
        "values": centred(seeds[2], (SEQUENCE_TOKENS, KEY_VALUE_HEADS * HEAD_WIDTH), 1.0, 6.0, ((0, 16), (1, 2))),
        "span_table": draw_span_table(jax.random.fold_in(seeds[6], 71), 0),
        "doc_ids": jnp.searchsorted(jnp.cumsum(ragged_sizes(seeds[4], DOCS, SEQUENCE_TOKENS, SEQUENCE_TOKENS // 4, 2)), jnp.arange(SEQUENCE_TOKENS), side="right").astype(jnp.int32),
        "out_weight": centred(seeds[5], (QUERY_HEADS * HEAD_WIDTH, D), (QUERY_HEADS * HEAD_WIDTH) ** -0.5, 0.09375, ((0, 2),)),
    }


def reference(queries, keys, values, span_table, doc_ids, out_weight):
    query_group = QUERY_HEADS // KEY_VALUE_HEADS
    scale = HEAD_WIDTH ** -0.5
    rows = jnp.arange(SEQUENCE_TOKENS, dtype=jnp.int32)
    positions = (span_table[rows // SPAN_TOKENS] * SPAN_TOKENS + rows % SPAN_TOKENS).astype(jnp.int32)
    documents = doc_ids[positions]
    key_head_rows = keys.reshape(SEQUENCE_TOKENS, KEY_VALUE_HEADS, HEAD_WIDTH).astype(jnp.float32)
    value_head_rows = values.reshape(SEQUENCE_TOKENS, KEY_VALUE_HEADS, HEAD_WIDTH).astype(jnp.float32)

    def block(index):
        first = (index * SPAN_TOKENS).astype(jnp.int32)
        query_matrix = lax.dynamic_slice_in_dim(queries, first, SPAN_TOKENS, 0)
        query_matrix = query_matrix.reshape(SPAN_TOKENS, KEY_VALUE_HEADS, query_group, HEAD_WIDTH).astype(jnp.float32)
        query_pos = lax.dynamic_slice_in_dim(positions, first, SPAN_TOKENS, 0)
        query_doc = lax.dynamic_slice_in_dim(documents, first, SPAN_TOKENS, 0)
        visible = (positions[None, :] <= query_pos[:, None]) & (documents[None, :] == query_doc[:, None])
        scores = jnp.einsum("qkgd,nkd->kgqn", query_matrix, key_head_rows) * scale
        scores = jnp.where(visible, scores, -1e30)
        best = jnp.max(scores, axis=-1, keepdims=True)
        weights = jnp.where(visible, jnp.exp(scores - best), 0.0)
        denom = jnp.sum(weights, axis=-1)
        rounded = lax.optimization_barrier(weights.astype(jnp.bfloat16)).astype(jnp.float32)
        numer = jnp.einsum("kgqn,nkd->kgqd", rounded, value_head_rows)
        result = numer / denom[..., None]
        return result.transpose(2, 0, 1, 3).reshape(SPAN_TOKENS, QUERY_HEADS * HEAD_WIDTH).astype(jnp.bfloat16)

    attn = lax.map(block, jnp.arange(SEQUENCE_TOKENS // SPAN_TOKENS, dtype=jnp.int32)).reshape(SEQUENCE_TOKENS, QUERY_HEADS * HEAD_WIDTH)
    return jnp.dot(attn, out_weight, preferred_element_type=jnp.float32).astype(jnp.bfloat16)
```

```python
import functools
import math

import jax
import jax.numpy as jnp
from jax import lax
from jax.experimental import pallas as pl
from jax.experimental.pallas import tpu as pltpu
from jax.sharding import PartitionSpec as P

HEAD_WIDTH = 128
DOCS = 8
LANES = 256
NEG = -1e30
MESH = pl.DeviceIdType.MESH


def kernel(
    line, q_ref, span_ref, doc_ref, k_hbm, v_hbm, w_hbm, out_ref,
    kv, w_vmem, q_t, acc, best, total, bias, low, high, attn, outgoing, incoming, kept,
    load_sem, w_sem, send0, send_z, send_xy, recv, out_send, out_recv,
):
    rows = q_ref.shape[0]
    span_len = rows // 2
    kv_heads = k_hbm.shape[1] // HEAD_WIDTH
    group = q_ref.shape[1] // HEAD_WIDTH // kv_heads
    tiles = group * rows // LANES
    third, sixth = rows // 3, rows // 6
    me = lax.axis_index("cp")
    hd = lax.axis_index("hd")
    z = me // 4
    y = (me // 2) % 2
    x = me % 2

    def slot(zz, fx, fy):
        xx = 1 - x if fx else x
        yy = 1 - y if fy else y
        return zz * 4 + yy * 2 + xx

    piece_rows = {
        "A": (0, third, 0), "B": (third, third, 1), "C": (2 * third, third, 2),
        "C0": (2 * third, sixth, 2), "C1": (2 * third + sixth, sixth, 3),
    }

    def part(src, piece):
        start, size, _ = piece_rows[piece]
        return kv.at[src, :, pl.ds(start, size), :]

    def copy_of(src, piece, target, sem):
        return pltpu.make_async_remote_copy(
            src_ref=part(src, piece), dst_ref=part(src, piece), send_sem=sem,
            recv_sem=recv.at[src, piece_rows[piece][2]],
            device_id={"cp": target}, device_id_type=MESH,
        )

    def arrived(src, piece):
        copy_of(src, piece, slot(z, True, False), send0.at[0]).wait_recv()

    to_x, to_y = slot(z, True, False), slot(z, False, True)
    up, down = me + 4, me - 4
    has_up, has_down = z < line - 1, z > 0

    loads = [
        pltpu.make_async_copy(k_hbm, kv.at[me, 0], load_sem.at[0]),
        pltpu.make_async_copy(v_hbm, kv.at[me, 1], load_sem.at[1]),
    ]
    w_load = pltpu.make_async_copy(w_hbm, w_vmem, w_sem)
    for load in loads:
        load.start()
    barrier = pltpu.get_barrier_semaphore()
    for target in (to_x, to_y):
        pl.semaphore_signal(barrier, inc=1, device_id={"cp": target}, device_id_type=MESH)
    pl.semaphore_signal(barrier, inc=1, device_id={"hd": 1 - hd}, device_id_type=MESH)

    @pl.when(has_up)
    def _():
        pl.semaphore_signal(barrier, inc=1, device_id={"cp": up}, device_id_type=MESH)

    @pl.when(has_down)
    def _():
        pl.semaphore_signal(barrier, inc=1, device_id={"cp": down}, device_id_type=MESH)

    pl.semaphore_wait(barrier, 3 + has_up.astype(jnp.int32) + has_down.astype(jnp.int32))
    for load in loads:
        load.wait()

    own, xn, yn, dg = (False, False), (True, False), (False, True), (True, True)
    first_x = [(own, "A"), (own, "C"), (own, "B")]
    first_y = [(own, "B"), (own, "C"), (own, "A")]
    first_z = [(own, "C"), (own, "A"), (own, "B")]
    later_z = [(xn, "A"), (yn, "B")]

    def first_stage(act, xs, ys, zs, nx, ny, nz):
        for i in range(max(len(xs), len(ys))):
            if i < len(xs):
                act(copy_of(slot(z, *xs[i][0]), xs[i][1], to_x, send0.at[nx + i]))
            if i < len(ys):
                act(copy_of(slot(z, *ys[i][0]), ys[i][1], to_y, send0.at[5 + ny + i]))

        @pl.when(has_up)
        def _():
            for i, (flips, piece) in enumerate(zs):
                act(copy_of(slot(z, *flips), piece, up, send0.at[10 + nz + i]))

        @pl.when(has_down)
        def _():
            for i, (flips, piece) in enumerate(zs):
                act(copy_of(slot(z, *flips), piece, down, send0.at[15 + nz + i]))

    def go(copy):
        copy.start()

    def sent(copy):
        copy.wait_send()

    first_stage(go, first_x, first_y, first_z, 0, 0, 0)
    w_load.start()

    lane = lax.broadcasted_iota(jnp.int32, (1, tiles * LANES), 1) % rows
    span0, span1 = span_ref[2 * me], span_ref[2 * me + 1]
    row_pos = jnp.where(lane < span_len, span0 * span_len + lane, (span1 - 1) * span_len + lane)
    row_pos = row_pos.astype(jnp.float32)
    row_low = jnp.zeros_like(row_pos)
    docs = doc_ref[...]
    for d in range(1, DOCS):
        start = jnp.sum(jnp.where(docs < d, 1.0, 0.0), keepdims=True)
        row_low = jnp.maximum(row_low, jnp.where(start <= row_pos, start, 0.0))
    for c in range(tiles):
        low[c] = row_low[:, c * LANES:(c + 1) * LANES]
        high[c] = row_pos[:, c * LANES:(c + 1) * LANES]
    for g in range(kv_heads):
        heads = [q_ref[:, (g * group + h) * HEAD_WIDTH:(g * group + h + 1) * HEAD_WIDTH] for h in range(group)]
        flipped = jnp.concatenate(heads, axis=0).T
        for c in range(tiles):
            q_t[g, c] = flipped[:, c * LANES:(c + 1) * LANES]

    factor = HEAD_WIDTH ** (-0.5) * math.log2(math.e)

    def attend(src, initial=False):
        s0, s1 = span_ref[2 * src], span_ref[2 * src + 1]
        key = lax.broadcasted_iota(jnp.int32, (rows, LANES), 0)
        key_pos = jnp.where(key < span_len, s0 * span_len, (s1 - 1) * span_len) + key
        key_pos = key_pos.astype(jnp.float32)
        for c in range(tiles):
            visible = (key_pos >= low[c]) & (key_pos <= high[c])
            bias[c] = jnp.where(visible, 0.0, NEG)

        @pl.loop(0, kv_heads)
        def _(g):
            columns = pl.ds(pl.multiple_of(g * HEAD_WIDTH, HEAD_WIDTH), HEAD_WIDTH)
            keys = kv[src, 0, :, columns]
            values = kv[src, 1, :, columns]
            for c in range(tiles):
                scores = jnp.dot(keys, q_t[g, c], preferred_element_type=jnp.float32)
                scores = scores * factor + bias[c]
                top = jnp.max(scores, axis=0, keepdims=True)
                if not initial:
                    old = best[g, c]
                    top = jnp.maximum(old, top)
                    fade = jnp.exp2(old - top)
                weights = jnp.exp2(scores - top)
                weight_sum = jnp.sum(weights, axis=0, keepdims=True)
                part_sum = lax.dot_general(
                    values, weights.astype(jnp.bfloat16), (((0,), (0,)), ((), ())),
                    preferred_element_type=jnp.float32,
                )
                best[g, c] = top
                if initial:
                    total[g, c] = weight_sum
                    acc[g, c] = part_sum
                else:
                    total[g, c] = total[g, c] * fade + weight_sum
                    acc[g, c] = acc[g, c] * fade + part_sum

    attend(me, initial=True)

    arrived(slot(z, *xn), "A")
    arrived(slot(z, *yn), "B")
    first_stage(go, [(yn, "B")], [(xn, "A")], later_z, 3, 3, 3)
    arrived(slot(z, *xn), "C")
    arrived(slot(z, *yn), "C")
    first_stage(go, [(yn, "C0")], [(xn, "C1")], [], 4, 4, 0)
    arrived(slot(z, *xn), "B")
    attend(slot(z, *xn))
    arrived(slot(z, *yn), "A")
    attend(slot(z, *yn))

    near = jnp.minimum(z, line - 1 - z)

    def plane(j):
        both = jnp.where(j % 2 == 1, z + (j + 1) // 2, z - j // 2)
        rest = jnp.where(z < line - 1 - z, j, line - 1 - j)
        return jnp.where(j <= 2 * near, both, rest)

    def sides(i, fn):
        @pl.when(z - i >= 0)
        def _():
            fn(z - i, 0, has_up, up)

        @pl.when(z + i < line)
        def _():
            fn(z + i, 1, has_down, down)

    z_pieces = [(own, "C", "xy"), (own, "A", "y"), (own, "B", "x"), (xn, "A", "y"), (yn, "B", "x")]

    def z_step(i, n, act):
        flips, piece, links = z_pieces[n]

        def fn(zz, side, can, target):
            src = slot(zz, *flips)
            if act is go:
                arrived(src, piece)

            @pl.when(can)
            def _():
                act(copy_of(src, piece, target, send_z.at[i - 1, side, n]))

            if "x" in links:
                act(copy_of(src, piece, to_x, send_xy.at[i - 1, side, 0, min(n, 2)
                                                         if n != 4 else 1]))
            if "y" in links:
                act(copy_of(src, piece, to_y, send_xy.at[i - 1, side, 1, min(n, 2)]))

        sides(i, fn)

    def corner_step(i, act):
        def fn(zz, side, can, target):
            src_x, src_y = slot(zz, *xn), slot(zz, *yn)
            if act is go:
                arrived(src_x, "C")
            act(copy_of(src_x, "C1", to_y, send_xy.at[i - 1, side, 1, 3]))
            if act is go:
                arrived(src_y, "C")
            act(copy_of(src_y, "C0", to_x, send_xy.at[i - 1, side, 0, 3]))

        sides(i, fn)

    def wait_step(i, flips, pieces):
        def fn(zz, side, can, target):
            for piece in pieces:
                arrived(slot(zz, *flips), piece)

        sides(i, fn)

    dg_pieces = ("B", "A", "C0", "C1")

    for piece in dg_pieces:
        arrived(slot(z, *dg), piece)
    attend(slot(z, *dg))

    def stage(i, carry):
        for n in range(3):
            z_step(i, n, go)
        here = plane(i)
        attend(slot(here, *own))
        z_step(i, 3, go)
        z_step(i, 4, go)
        corner_step(i, go)
        wait_step(i, xn, ("B",))
        attend(slot(here, *xn))
        wait_step(i, yn, ("A",))
        attend(slot(here, *yn))
        wait_step(i, dg, dg_pieces)
        attend(slot(here, *dg))
        return carry

    lax.fori_loop(1, line, stage, 0)

    for g in range(kv_heads):
        parts = [acc[g, c] / total[g, c] for c in range(tiles)]
        turned = jnp.concatenate(parts, axis=1).T.astype(jnp.bfloat16)
        for h in range(group):
            first = (g * group + h) * HEAD_WIDTH
            attn[:, first:first + HEAD_WIDTH] = turned[h * rows:(h + 1) * rows]

    w_load.wait()
    half = rows // 2
    count, width = outgoing.shape[0], outgoing.shape[2]

    def hand_over(n):
        return pltpu.make_async_remote_copy(
            src_ref=outgoing.at[n], dst_ref=incoming.at[n], send_sem=out_send.at[n],
            recv_sem=out_recv.at[n], device_id={"hd": 1 - hd}, device_id_type=MESH,
        )

    @pl.loop(0, count)
    def _(n):
        columns = pl.ds(pl.multiple_of(n * width, width), width)
        product = jnp.dot(attn[...], w_vmem[:, columns], preferred_element_type=jnp.float32)
        upper, lower = product[:half], product[half:]
        mine = hd == 0
        outgoing[n] = jnp.where(mine, lower, upper).astype(jnp.bfloat16)
        kept[n] = jnp.where(mine, upper, lower)
        hand_over(n).start()

    for n in range(count):
        hand_over(n).wait_recv()
        out_ref[:, n * width:(n + 1) * width] = (kept[n] + incoming[n].astype(jnp.float32)).astype(jnp.bfloat16)

    for n in range(count):
        hand_over(n).wait_send()
    first_stage(sent, first_x, first_y, first_z, 0, 0, 0)
    first_stage(sent, [(yn, "B")], [(xn, "A")], later_z, 3, 3, 3)
    first_stage(sent, [(yn, "C0")], [(xn, "C1")], [], 4, 4, 0)

    def drain(i, carry):
        for n in range(5):
            z_step(i, n, sent)
        corner_step(i, sent)
        return carry

    lax.fori_loop(1, line, drain, 0)


def local(cp, queries, keys, values, span_table, doc_ids, out_weight):
    rows = queries.shape[0]
    kv_heads = keys.shape[1] // HEAD_WIDTH
    group = queries.shape[1] // HEAD_WIDTH // kv_heads
    tiles = group * rows // LANES
    line = cp // 4
    model = out_weight.shape[1]
    count = 8
    width = model // count
    half = rows // 2
    vmem, hbm = pltpu.VMEM, pl.ANY
    spec = lambda space: pl.BlockSpec(memory_space=space)
    dma = pltpu.SemaphoreType.DMA
    f32, bf16 = jnp.float32, jnp.bfloat16
    return pl.pallas_call(
        functools.partial(kernel, line),
        out_shape=jax.ShapeDtypeStruct((half, model), bf16),
        in_specs=[spec(vmem), spec(pltpu.SMEM), spec(vmem), spec(hbm), spec(hbm), spec(hbm)],
        out_specs=spec(vmem),
        scratch_shapes=[
            vmem((cp, 2, rows, keys.shape[1]), bf16),
            vmem(out_weight.shape, bf16),
            vmem((kv_heads, tiles, HEAD_WIDTH, LANES), bf16),
            vmem((kv_heads, tiles, HEAD_WIDTH, LANES), f32),
            vmem((kv_heads, tiles, 1, LANES), f32),
            vmem((kv_heads, tiles, 1, LANES), f32),
            vmem((tiles, rows, LANES), f32),
            vmem((tiles, 1, LANES), f32),
            vmem((tiles, 1, LANES), f32),
            vmem((rows, queries.shape[1]), bf16),
            vmem((count, half, width), bf16),
            vmem((count, half, width), bf16),
            vmem((count, half, width), f32),
            dma((2,)), dma, dma((20,)), dma((line, 2, 5)), dma((line, 2, 2, 4)),
            dma((cp, 4)), dma((count,)), dma((count,)),
        ],
        compiler_params=pltpu.CompilerParams(
            collective_id=0, has_side_effects=True, vmem_limit_bytes=60 * 2 ** 20,
        ),
    )(queries, span_table, doc_ids.reshape(-1, 128), keys, values, out_weight)


def solution(mesh):
    return jax.shard_map(
        functools.partial(local, mesh.shape["cp"]),
        mesh=mesh,
        in_specs=(P("cp", "hd"), P("cp", "hd"), P("cp", "hd"), P(), P(), P("hd", None)),
        out_specs=P(("cp", "hd"), None),
        check_vma=False,
    )
```

```python
import functools
import math

import jax
import jax.numpy as jnp
from jax import lax
from jax.experimental import pallas as pl
from jax.experimental.pallas import tpu as pltpu
from jax.sharding import PartitionSpec as P

HEAD_WIDTH = 128
DOCS = 8
LANES = 256
NEG = -1e30
MESH = pl.DeviceIdType.MESH


def kernel(
    line, q_ref, span_ref, doc_ref, k_hbm, v_hbm, w_hbm, out_ref,
    kv, w_vmem, q_t, acc, best, total, fades, held, bias, low, high, attn, outgoing, incoming, kept,
    load_sem, w_sem, send0, send_z, send_xy, recv, out_send, out_recv,
):
    rows = q_ref.shape[0]
    span_len = rows // 2
    kv_heads = k_hbm.shape[1] // HEAD_WIDTH
    group = q_ref.shape[1] // HEAD_WIDTH // kv_heads
    tiles = group * rows // LANES
    third, sixth = rows // 3, rows // 6
    me = lax.axis_index("cp")
    hd = lax.axis_index("hd")
    z = me // 4
    y = (me // 2) % 2
    x = me % 2

    def slot(zz, fx, fy):
        xx = 1 - x if fx else x
        yy = 1 - y if fy else y
        return zz * 4 + yy * 2 + xx

    piece_rows = {
        "A": (0, third, 0), "B": (third, third, 1), "C": (2 * third, third, 2),
        "C0": (2 * third, sixth, 2), "C1": (2 * third + sixth, sixth, 3),
    }

    def part(src, piece):
        start, size, _ = piece_rows[piece]
        return kv.at[src, :, pl.ds(start, size), :]

    def copy_of(src, piece, target, sem):
        return pltpu.make_async_remote_copy(
            src_ref=part(src, piece), dst_ref=part(src, piece), send_sem=sem,
            recv_sem=recv.at[src, piece_rows[piece][2]],
            device_id={"cp": target}, device_id_type=MESH,
        )

    def arrived(src, piece):
        copy_of(src, piece, slot(z, True, False), send0.at[0]).wait_recv()

    to_x, to_y = slot(z, True, False), slot(z, False, True)
    up, down = me + 4, me - 4
    has_up, has_down = z < line - 1, z > 0

    loads = [
        pltpu.make_async_copy(k_hbm, kv.at[me, 0], load_sem.at[0]),
        pltpu.make_async_copy(v_hbm, kv.at[me, 1], load_sem.at[1]),
    ]
    w_load = pltpu.make_async_copy(w_hbm, w_vmem, w_sem)
    for load in loads:
        load.start()
    barrier = pltpu.get_barrier_semaphore()
    for target in (to_x, to_y):
        pl.semaphore_signal(barrier, inc=1, device_id={"cp": target}, device_id_type=MESH)
    pl.semaphore_signal(barrier, inc=1, device_id={"hd": 1 - hd}, device_id_type=MESH)

    @pl.when(has_up)
    def _():
        pl.semaphore_signal(barrier, inc=1, device_id={"cp": up}, device_id_type=MESH)

    @pl.when(has_down)
    def _():
        pl.semaphore_signal(barrier, inc=1, device_id={"cp": down}, device_id_type=MESH)

    pl.semaphore_wait(barrier, 3 + has_up.astype(jnp.int32) + has_down.astype(jnp.int32))
    for load in loads:
        load.wait()

    own, xn, yn, dg = (False, False), (True, False), (False, True), (True, True)
    first_x = [(own, "A"), (own, "C"), (own, "B")]
    first_y = [(own, "B"), (own, "C"), (own, "A")]
    first_z = [(own, "C"), (own, "A"), (own, "B")]
    later_z = [(xn, "A"), (yn, "B")]

    def first_stage(act, xs, ys, zs, nx, ny, nz):
        for i in range(max(len(xs), len(ys))):
            if i < len(xs):
                act(copy_of(slot(z, *xs[i][0]), xs[i][1], to_x, send0.at[nx + i]))
            if i < len(ys):
                act(copy_of(slot(z, *ys[i][0]), ys[i][1], to_y, send0.at[5 + ny + i]))

        @pl.when(has_up)
        def _():
            for i, (flips, piece) in enumerate(zs):
                act(copy_of(slot(z, *flips), piece, up, send0.at[10 + nz + i]))

        @pl.when(has_down)
        def _():
            for i, (flips, piece) in enumerate(zs):
                act(copy_of(slot(z, *flips), piece, down, send0.at[15 + nz + i]))

    def go(copy):
        copy.start()

    def sent(copy):
        copy.wait_send()

    first_stage(go, first_x, first_y, first_z, 0, 0, 0)
    w_load.start()

    lane = lax.broadcasted_iota(jnp.int32, (1, tiles * LANES), 1) % rows
    span0, span1 = span_ref[2 * me], span_ref[2 * me + 1]
    row_pos = jnp.where(lane < span_len, span0 * span_len + lane, (span1 - 1) * span_len + lane)
    row_pos = row_pos.astype(jnp.float32)
    row_low = jnp.zeros_like(row_pos)
    docs = doc_ref[...]
    for d in range(1, DOCS):
        start = jnp.sum(jnp.where(docs < d, 1.0, 0.0), keepdims=True)
        row_low = jnp.maximum(row_low, jnp.where(start <= row_pos, start, 0.0))
    for c in range(tiles):
        low[c] = row_low[:, c * LANES:(c + 1) * LANES]
        high[c] = row_pos[:, c * LANES:(c + 1) * LANES]
    for g in range(kv_heads):
        heads = [q_ref[:, (g * group + h) * HEAD_WIDTH:(g * group + h + 1) * HEAD_WIDTH] for h in range(group)]
        flipped = jnp.concatenate(heads, axis=0).T
        for c in range(tiles):
            q_t[g, c] = flipped[:, c * LANES:(c + 1) * LANES]

    factor = HEAD_WIDTH ** (-0.5) * math.log2(math.e)

    def attend(src, initial=False):
        s0, s1 = span_ref[2 * src], span_ref[2 * src + 1]
        key = lax.broadcasted_iota(jnp.int32, (rows, LANES), 0)
        key_pos = jnp.where(key < span_len, s0 * span_len, (s1 - 1) * span_len) + key
        key_pos = key_pos.astype(jnp.float32)
        for c in range(tiles):
            visible = (key_pos >= low[c]) & (key_pos <= high[c])
            bias[c] = jnp.where(visible, 0.0, NEG)

        def weigh(g):
            keys = kv[src, 0, :, g * HEAD_WIDTH:(g + 1) * HEAD_WIDTH]
            for c in range(tiles):
                scores = jnp.dot(keys, q_t[g, c], preferred_element_type=jnp.float32)
                scores = scores * factor + bias[c]
                top = jnp.max(scores, axis=0, keepdims=True)
                if not initial:
                    old = best[g, c]
                    top = jnp.maximum(old, top)
                    fade = jnp.exp2(old - top)
                    fades[g, c] = fade
                weights = jnp.exp2(scores - top)
                weight_sum = jnp.sum(weights, axis=0, keepdims=True)
                best[g, c] = top
                total[g, c] = weight_sum if initial else total[g, c] * fade + weight_sum
                held[g, c] = weights.astype(jnp.bfloat16)

        def gather(g):
            values = kv[src, 1, :, g * HEAD_WIDTH:(g + 1) * HEAD_WIDTH].T
            for c in range(tiles):
                part_sum = jnp.dot(values, held[g, c], preferred_element_type=jnp.float32)
                acc[g, c] = part_sum if initial else acc[g, c] * fades[g, c] + part_sum

        for g in range(kv_heads):
            weigh(g)
            if g:
                gather(g - 1)
        gather(kv_heads - 1)

    attend(me, initial=True)

    arrived(slot(z, *xn), "A")
    arrived(slot(z, *yn), "B")
    first_stage(go, [(yn, "B")], [(xn, "A")], later_z, 3, 3, 3)
    arrived(slot(z, *xn), "C")
    arrived(slot(z, *yn), "C")
    first_stage(go, [(yn, "C0")], [(xn, "C1")], [], 4, 4, 0)
    arrived(slot(z, *xn), "B")
    attend(slot(z, *xn))
    arrived(slot(z, *yn), "A")
    attend(slot(z, *yn))

    near = jnp.minimum(z, line - 1 - z)

    def plane(j):
        both = jnp.where(j % 2 == 1, z + (j + 1) // 2, z - j // 2)
        rest = jnp.where(z < line - 1 - z, j, line - 1 - j)
        return jnp.where(j <= 2 * near, both, rest)

    def sides(i, fn):
        @pl.when(z - i >= 0)
        def _():
            fn(z - i, 0, has_up, up)

        @pl.when(z + i < line)
        def _():
            fn(z + i, 1, has_down, down)

    z_pieces = [(own, "C", "xy"), (own, "A", "y"), (own, "B", "x"), (xn, "A", "y"), (yn, "B", "x")]

    def z_step(i, n, act):
        flips, piece, links = z_pieces[n]

        def fn(zz, side, can, target):
            src = slot(zz, *flips)
            if act is go:
                arrived(src, piece)

            @pl.when(can)
            def _():
                act(copy_of(src, piece, target, send_z.at[i - 1, side, n]))

            if "x" in links:
                act(copy_of(src, piece, to_x, send_xy.at[i - 1, side, 0, min(n, 2)
                                                         if n != 4 else 1]))
            if "y" in links:
                act(copy_of(src, piece, to_y, send_xy.at[i - 1, side, 1, min(n, 2)]))

        sides(i, fn)

    def corner_step(i, act):
        def fn(zz, side, can, target):
            src_x, src_y = slot(zz, *xn), slot(zz, *yn)
            if act is go:
                arrived(src_x, "C")
            act(copy_of(src_x, "C1", to_y, send_xy.at[i - 1, side, 1, 3]))
            if act is go:
                arrived(src_y, "C")
            act(copy_of(src_y, "C0", to_x, send_xy.at[i - 1, side, 0, 3]))

        sides(i, fn)

    def wait_step(i, flips, pieces):
        def fn(zz, side, can, target):
            for piece in pieces:
                arrived(slot(zz, *flips), piece)

        sides(i, fn)

    dg_pieces = ("B", "A", "C0", "C1")

    for piece in dg_pieces:
        arrived(slot(z, *dg), piece)
    attend(slot(z, *dg))

    def stage(i, carry):
        for n in range(3):
            z_step(i, n, go)
        here = plane(i)
        attend(slot(here, *own))
        z_step(i, 3, go)
        z_step(i, 4, go)
        corner_step(i, go)
        wait_step(i, xn, ("B",))
        attend(slot(here, *xn))
        wait_step(i, yn, ("A",))
        attend(slot(here, *yn))
        wait_step(i, dg, dg_pieces)
        attend(slot(here, *dg))
        return carry

    lax.fori_loop(1, line, stage, 0)

    for g in range(kv_heads):
        parts = [acc[g, c] / total[g, c] for c in range(tiles)]
        turned = jnp.concatenate(parts, axis=1).T.astype(jnp.bfloat16)
        for h in range(group):
            first = (g * group + h) * HEAD_WIDTH
            attn[:, first:first + HEAD_WIDTH] = turned[h * rows:(h + 1) * rows]

    w_load.wait()
    half = rows // 2
    count, width = outgoing.shape[0], outgoing.shape[2]

    def hand_over(n):
        return pltpu.make_async_remote_copy(
            src_ref=outgoing.at[n], dst_ref=incoming.at[n], send_sem=out_send.at[n],
            recv_sem=out_recv.at[n], device_id={"hd": 1 - hd}, device_id_type=MESH,
        )

    @pl.loop(0, count)
    def _(n):
        columns = pl.ds(pl.multiple_of(n * width, width), width)
        product = jnp.dot(attn[...], w_vmem[:, columns], preferred_element_type=jnp.float32)
        upper, lower = product[:half], product[half:]
        mine = hd == 0
        outgoing[n] = jnp.where(mine, lower, upper).astype(jnp.bfloat16)
        kept[n] = jnp.where(mine, upper, lower)
        hand_over(n).start()

    for n in range(count):
        hand_over(n).wait_recv()
        out_ref[:, n * width:(n + 1) * width] = (kept[n] + incoming[n].astype(jnp.float32)).astype(jnp.bfloat16)

    for n in range(count):
        hand_over(n).wait_send()
    first_stage(sent, first_x, first_y, first_z, 0, 0, 0)
    first_stage(sent, [(yn, "B")], [(xn, "A")], later_z, 3, 3, 3)
    first_stage(sent, [(yn, "C0")], [(xn, "C1")], [], 4, 4, 0)

    def drain(i, carry):
        for n in range(5):
            z_step(i, n, sent)
        corner_step(i, sent)
        return carry

    lax.fori_loop(1, line, drain, 0)


def local(cp, queries, keys, values, span_table, doc_ids, out_weight):
    rows = queries.shape[0]
    kv_heads = keys.shape[1] // HEAD_WIDTH
    group = queries.shape[1] // HEAD_WIDTH // kv_heads
    tiles = group * rows // LANES
    line = cp // 4
    model = out_weight.shape[1]
    count = 8
    width = model // count
    half = rows // 2
    vmem, hbm = pltpu.VMEM, pl.ANY
    spec = lambda space: pl.BlockSpec(memory_space=space)
    dma = pltpu.SemaphoreType.DMA
    f32, bf16 = jnp.float32, jnp.bfloat16
    return pl.pallas_call(
        functools.partial(kernel, line),
        out_shape=jax.ShapeDtypeStruct((half, model), bf16),
        in_specs=[spec(vmem), spec(pltpu.SMEM), spec(vmem), spec(hbm), spec(hbm), spec(hbm)],
        out_specs=spec(vmem),
        scratch_shapes=[
            vmem((cp, 2, rows, keys.shape[1]), bf16),
            vmem(out_weight.shape, bf16),
            vmem((kv_heads, tiles, HEAD_WIDTH, LANES), bf16),
            vmem((kv_heads, tiles, HEAD_WIDTH, LANES), f32),
            vmem((kv_heads, tiles, 1, LANES), f32),
            vmem((kv_heads, tiles, 1, LANES), f32),
            vmem((kv_heads, tiles, 1, LANES), f32),
            vmem((kv_heads, tiles, rows, LANES), bf16),
            vmem((tiles, rows, LANES), f32),
            vmem((tiles, 1, LANES), f32),
            vmem((tiles, 1, LANES), f32),
            vmem((rows, queries.shape[1]), bf16),
            vmem((count, half, width), bf16),
            vmem((count, half, width), bf16),
            vmem((count, half, width), f32),
            dma((2,)), dma, dma((20,)), dma((line, 2, 5)), dma((line, 2, 2, 4)),
            dma((cp, 4)), dma((count,)), dma((count,)),
        ],
        compiler_params=pltpu.CompilerParams(
            collective_id=0, has_side_effects=True, vmem_limit_bytes=60 * 2 ** 20,
        ),
    )(queries, span_table, doc_ids.reshape(-1, 128), keys, values, out_weight)


def solution(mesh):
    return jax.shard_map(
        functools.partial(local, mesh.shape["cp"]),
        mesh=mesh,
        in_specs=(P("cp", "hd"), P("cp", "hd"), P("cp", "hd"), P(), P(), P("hd", None)),
        out_specs=P(("cp", "hd"), None),
        check_vma=False,
    )
```

```python
import functools
import math

import jax
import jax.numpy as jnp
from jax import lax
from jax.experimental import pallas as pl
from jax.experimental.pallas import tpu as pltpu
from jax.sharding import PartitionSpec as P

HEAD_WIDTH = 128
DOCS = 8
LANES = 256
NEG = -1e30
MESH = pl.DeviceIdType.MESH


def kernel(
    line, q_ref, span_ref, doc_ref, k_hbm, v_hbm, w_hbm, out_ref,
    kv, w_vmem, q_t, acc, best, total, fades, held, bias, low, high, attn, outgoing, incoming, kept,
    load_sem, w_sem, send0, send_z, send_xy, recv, out_send, out_recv,
):
    rows = q_ref.shape[0]
    span_len = rows // 2
    kv_heads = k_hbm.shape[1] // HEAD_WIDTH
    group = q_ref.shape[1] // HEAD_WIDTH // kv_heads
    tiles = group * rows // LANES
    whole = rows // 3
    side = (rows - whole) // 2
    me = lax.axis_index("cp")
    hd = lax.axis_index("hd")
    z = me // 4
    y = (me // 2) % 2
    x = me % 2

    def slot(zz, fx, fy):
        xx = 1 - x if fx else x
        yy = 1 - y if fy else y
        return zz * 4 + yy * 2 + xx

    piece_rows = {
        "A": (0, side, 0), "B": (side, side, 1), "C": (2 * side, whole, 2),
        "C0": (2 * side, whole // 2, 2), "C1": (2 * side + whole // 2, whole // 2, 3),
    }

    def part(src, piece):
        start, size, _ = piece_rows[piece]
        return kv.at[src, :, pl.ds(start, size), :]

    def copy_of(src, piece, target, sem):
        return pltpu.make_async_remote_copy(
            src_ref=part(src, piece), dst_ref=part(src, piece), send_sem=sem,
            recv_sem=recv.at[src, piece_rows[piece][2]],
            device_id={"cp": target}, device_id_type=MESH,
        )

    def arrived(src, piece):
        copy_of(src, piece, slot(z, True, False), send0.at[0]).wait_recv()

    to_x, to_y = slot(z, True, False), slot(z, False, True)
    up, down = me + 4, me - 4
    has_up, has_down = z < line - 1, z > 0

    loads = [
        pltpu.make_async_copy(k_hbm, kv.at[me, 0], load_sem.at[0]),
        pltpu.make_async_copy(v_hbm, kv.at[me, 1], load_sem.at[1]),
    ]
    w_load = pltpu.make_async_copy(w_hbm, w_vmem, w_sem)
    for load in loads:
        load.start()
    barrier = pltpu.get_barrier_semaphore()
    for target in (to_x, to_y):
        pl.semaphore_signal(barrier, inc=1, device_id={"cp": target}, device_id_type=MESH)
    pl.semaphore_signal(barrier, inc=1, device_id={"hd": 1 - hd}, device_id_type=MESH)

    @pl.when(has_up)
    def _():
        pl.semaphore_signal(barrier, inc=1, device_id={"cp": up}, device_id_type=MESH)

    @pl.when(has_down)
    def _():
        pl.semaphore_signal(barrier, inc=1, device_id={"cp": down}, device_id_type=MESH)

    pl.semaphore_wait(barrier, 3 + has_up.astype(jnp.int32) + has_down.astype(jnp.int32))
    for load in loads:
        load.wait()

    own, xn, yn, dg = (False, False), (True, False), (False, True), (True, True)
    first_x = [(own, "A"), (own, "C"), (own, "B")]
    first_y = [(own, "B"), (own, "C"), (own, "A")]
    first_z = [(own, "C"), (own, "A"), (own, "B")]
    later_z = [(xn, "A"), (yn, "B")]

    def first_stage(act, xs, ys, zs, nx, ny, nz):
        for i in range(max(len(xs), len(ys))):
            if i < len(xs):
                act(copy_of(slot(z, *xs[i][0]), xs[i][1], to_x, send0.at[nx + i]))
            if i < len(ys):
                act(copy_of(slot(z, *ys[i][0]), ys[i][1], to_y, send0.at[5 + ny + i]))

        @pl.when(has_up)
        def _():
            for i, (flips, piece) in enumerate(zs):
                act(copy_of(slot(z, *flips), piece, up, send0.at[10 + nz + i]))

        @pl.when(has_down)
        def _():
            for i, (flips, piece) in enumerate(zs):
                act(copy_of(slot(z, *flips), piece, down, send0.at[15 + nz + i]))

    def go(copy):
        copy.start()

    def sent(copy):
        copy.wait_send()

    first_stage(go, first_x, first_y, first_z, 0, 0, 0)
    w_load.start()

    lane = lax.broadcasted_iota(jnp.int32, (1, tiles * LANES), 1) % rows
    span0, span1 = span_ref[2 * me], span_ref[2 * me + 1]
    row_pos = jnp.where(lane < span_len, span0 * span_len + lane, (span1 - 1) * span_len + lane)
    row_pos = row_pos.astype(jnp.float32)
    row_low = jnp.zeros_like(row_pos)
    docs = doc_ref[...]
    for d in range(1, DOCS):
        start = jnp.sum(jnp.where(docs < d, 1.0, 0.0), keepdims=True)
        row_low = jnp.maximum(row_low, jnp.where(start <= row_pos, start, 0.0))
    for c in range(tiles):
        low[c] = row_low[:, c * LANES:(c + 1) * LANES]
        high[c] = row_pos[:, c * LANES:(c + 1) * LANES]
    for g in range(kv_heads):
        heads = [q_ref[:, (g * group + h) * HEAD_WIDTH:(g * group + h + 1) * HEAD_WIDTH] for h in range(group)]
        flipped = jnp.concatenate(heads, axis=0).T
        for c in range(tiles):
            q_t[g, c] = flipped[:, c * LANES:(c + 1) * LANES]

    factor = HEAD_WIDTH ** (-0.5) * math.log2(math.e)

    def attend(src, initial=False):
        s0, s1 = span_ref[2 * src], span_ref[2 * src + 1]
        key = lax.broadcasted_iota(jnp.int32, (rows, LANES), 0)
        key_pos = jnp.where(key < span_len, s0 * span_len, (s1 - 1) * span_len) + key
        key_pos = key_pos.astype(jnp.float32)
        for c in range(tiles):
            visible = (key_pos >= low[c]) & (key_pos <= high[c])
            bias[c] = jnp.where(visible, 0.0, NEG)

        def weigh(g):
            keys = kv[src, 0, :, g * HEAD_WIDTH:(g + 1) * HEAD_WIDTH]
            for c in range(tiles):
                scores = jnp.dot(keys, q_t[g, c], preferred_element_type=jnp.float32)
                scores = scores * factor + bias[c]
                top = jnp.max(scores, axis=0, keepdims=True)
                if not initial:
                    old = best[g, c]
                    top = jnp.maximum(old, top)
                    fade = jnp.exp2(old - top)
                    fades[g, c] = fade
                weights = jnp.exp2(scores - top)
                weight_sum = jnp.sum(weights, axis=0, keepdims=True)
                best[g, c] = top
                total[g, c] = weight_sum if initial else total[g, c] * fade + weight_sum
                held[g, c] = weights.astype(jnp.bfloat16)

        def gather(g):
            values = kv[src, 1, :, g * HEAD_WIDTH:(g + 1) * HEAD_WIDTH].T
            for c in range(tiles):
                part_sum = jnp.dot(values, held[g, c], preferred_element_type=jnp.float32)
                acc[g, c] = part_sum if initial else acc[g, c] * fades[g, c] + part_sum

        for g in range(kv_heads):
            weigh(g)
            if g:
                gather(g - 1)
        gather(kv_heads - 1)

    attend(me, initial=True)

    arrived(slot(z, *xn), "A")
    arrived(slot(z, *yn), "B")
    first_stage(go, [(yn, "B")], [(xn, "A")], later_z, 3, 3, 3)
    arrived(slot(z, *xn), "C")
    arrived(slot(z, *yn), "C")
    first_stage(go, [(yn, "C0")], [(xn, "C1")], [], 4, 4, 0)
    near = jnp.minimum(z, line - 1 - z)

    def plane(j):
        both = jnp.where(j % 2 == 1, z + (j + 1) // 2, z - j // 2)
        rest = jnp.where(z < line - 1 - z, j, line - 1 - j)
        return jnp.where(j <= 2 * near, both, rest)

    def sides(i, fn):
        @pl.when(z - i >= 0)
        def _():
            fn(z - i, 0, has_up, up)

        @pl.when((z + i < line) & (i > 0))
        def _():
            fn(z + i, 1, has_down, down)

    z_pieces = [(own, "C", "xy"), (own, "A", "y"), (own, "B", "x"), (xn, "A", "y"), (yn, "B", "x")]

    def z_step(i, n, act):
        flips, piece, links = z_pieces[n]

        def fn(zz, side, can, target):
            src = slot(zz, *flips)
            if act is go:
                arrived(src, piece)

            @pl.when(can)
            def _():
                act(copy_of(src, piece, target, send_z.at[i - 1, side, n]))

            if "x" in links:
                act(copy_of(src, piece, to_x, send_xy.at[i - 1, side, 0, min(n, 2)
                                                         if n != 4 else 1]))
            if "y" in links:
                act(copy_of(src, piece, to_y, send_xy.at[i - 1, side, 1, min(n, 2)]))

        sides(i, fn)

    def corner_step(i, act):
        def fn(zz, side, can, target):
            src_x, src_y = slot(zz, *xn), slot(zz, *yn)
            if act is go:
                arrived(src_x, "C")
            act(copy_of(src_x, "C1", to_y, send_xy.at[i - 1, side, 1, 3]))
            if act is go:
                arrived(src_y, "C")
            act(copy_of(src_y, "C0", to_x, send_xy.at[i - 1, side, 0, 3]))

        sides(i, fn)

    def wait_step(i, flips, pieces):
        def fn(zz, side, can, target):
            for piece in pieces:
                arrived(slot(zz, *flips), piece)

        sides(i, fn)

    dg_pieces = ("B", "A", "C0", "C1")

    def finish(i):
        here = plane(i)
        for flips, pieces in ((xn, ("B",)), (yn, ("A",)), (dg, dg_pieces)):
            wait_step(i, flips, pieces)
            attend(slot(here, *flips))

    def stage(i, carry, last=False):
        z_step(i, 0, go)
        z_step(i, 1, go)

        @pl.when(i > 1)
        def _():
            corner_step(i - 1, go)

        z_step(i, 2, go)
        if last:
            finish(i - 1)
            attend(slot(plane(i), *own))
        z_step(i, 3, go)
        z_step(i, 4, go)
        if not last:
            attend(slot(plane(i), *own))
            finish(i - 1)
        return carry

    lax.fori_loop(1, line - 1, stage, 0)
    stage(line - 1, 0, last=True)
    corner_step(line - 1, go)
    finish(line - 1)

    for g in range(kv_heads):
        parts = [acc[g, c] / total[g, c] for c in range(tiles)]
        turned = jnp.concatenate(parts, axis=1).T.astype(jnp.bfloat16)
        for h in range(group):
            first = (g * group + h) * HEAD_WIDTH
            attn[:, first:first + HEAD_WIDTH] = turned[h * rows:(h + 1) * rows]

    w_load.wait()
    half = rows // 2
    count, width = outgoing.shape[0], outgoing.shape[2]

    def hand_over(n):
        return pltpu.make_async_remote_copy(
            src_ref=outgoing.at[n], dst_ref=incoming.at[n], send_sem=out_send.at[n],
            recv_sem=out_recv.at[n], device_id={"hd": 1 - hd}, device_id_type=MESH,
        )

    @pl.loop(0, count)
    def _(n):
        columns = pl.ds(pl.multiple_of(n * width, width), width)
        product = jnp.dot(attn[...], w_vmem[:, columns], preferred_element_type=jnp.float32)
        upper, lower = product[:half], product[half:]
        mine = hd == 0
        outgoing[n] = jnp.where(mine, lower, upper).astype(jnp.bfloat16)
        kept[n] = jnp.where(mine, upper, lower)
        hand_over(n).start()

    for n in range(count):
        hand_over(n).wait_recv()
        out_ref[:, n * width:(n + 1) * width] = (kept[n] + incoming[n].astype(jnp.float32)).astype(jnp.bfloat16)

    for n in range(count):
        hand_over(n).wait_send()
    first_stage(sent, first_x, first_y, first_z, 0, 0, 0)
    first_stage(sent, [(yn, "B")], [(xn, "A")], later_z, 3, 3, 3)
    first_stage(sent, [(yn, "C0")], [(xn, "C1")], [], 4, 4, 0)

    def drain(i, carry):
        for n in range(5):
            z_step(i, n, sent)
        corner_step(i, sent)
        return carry

    lax.fori_loop(1, line, drain, 0)


def local(cp, queries, keys, values, span_table, doc_ids, out_weight):
    rows = queries.shape[0]
    kv_heads = keys.shape[1] // HEAD_WIDTH
    group = queries.shape[1] // HEAD_WIDTH // kv_heads
    tiles = group * rows // LANES
    line = cp // 4
    model = out_weight.shape[1]
    count = 8
    width = model // count
    half = rows // 2
    vmem, hbm = pltpu.VMEM, pl.ANY
    spec = lambda space: pl.BlockSpec(memory_space=space)
    dma = pltpu.SemaphoreType.DMA
    f32, bf16 = jnp.float32, jnp.bfloat16
    return pl.pallas_call(
        functools.partial(kernel, line),
        out_shape=jax.ShapeDtypeStruct((half, model), bf16),
        in_specs=[spec(vmem), spec(pltpu.SMEM), spec(vmem), spec(hbm), spec(hbm), spec(hbm)],
        out_specs=spec(vmem),
        scratch_shapes=[
            vmem((cp, 2, rows, keys.shape[1]), bf16),
            vmem(out_weight.shape, bf16),
            vmem((kv_heads, tiles, HEAD_WIDTH, LANES), bf16),
            vmem((kv_heads, tiles, HEAD_WIDTH, LANES), f32),
            vmem((kv_heads, tiles, 1, LANES), f32),
            vmem((kv_heads, tiles, 1, LANES), f32),
            vmem((kv_heads, tiles, 1, LANES), f32),
            vmem((kv_heads, tiles, rows, LANES), bf16),
            vmem((tiles, rows, LANES), f32),
            vmem((tiles, 1, LANES), f32),
            vmem((tiles, 1, LANES), f32),
            vmem((rows, queries.shape[1]), bf16),
            vmem((count, half, width), bf16),
            vmem((count, half, width), bf16),
            vmem((count, half, width), f32),
            dma((2,)), dma, dma((20,)), dma((line, 2, 5)), dma((line, 2, 2, 4)),
            dma((cp, 4)), dma((count,)), dma((count,)),
        ],
        compiler_params=pltpu.CompilerParams(
            collective_id=0, has_side_effects=True, vmem_limit_bytes=60 * 2 ** 20,
        ),
    )(queries, span_table, doc_ids.reshape(-1, 128), keys, values, out_weight)


def solution(mesh):
    return jax.shard_map(
        functools.partial(local, mesh.shape["cp"]),
        mesh=mesh,
        in_specs=(P("cp", "hd"), P("cp", "hd"), P("cp", "hd"), P(), P(), P("hd", None)),
        out_specs=P(("cp", "hd"), None),
        check_vma=False,
    )
```
